256 devices in a mesh: dp: 16 (over z_hi, x, core), space: 16 (over y, z_lo).
Axes of the slice: x: 4, y: 4, z: 8 (z_hi: 2, z_lo: 4; z = z_hi * 4 + z_lo), core: 2. Of those that a mesh axis runs over, the one named last changes fastest.
Arguments:
- section_three: bfloat16 [16, 128, 128, 512], P('dp', 'space'), parts along dimension 0, may hold values from -6 to 6
- section_four: bfloat16 [16, 64, 64, 1024], P('dp', 'space'), parts along dimension 0, may hold values from -6 to 6
- section_five: bfloat16 [16, 32, 32, 2048], P('dp', 'space'), parts along dimension 0, may hold values from -6 to 6
- lateral_three: bfloat16 [512, 256], P('space'), may hold values from -0.25 to 0.25
- lateral_four: bfloat16 [1024, 256], P('space'), may hold values from -0.1875 to 0.1875
- lateral_five: bfloat16 [2048, 256], P('space'), may hold values from -0.125 to 0.125
- lateral_bias_three: float32 [256], replicated, may hold values from -3 to 3
- lateral_bias_four: float32 [256], replicated, may hold values from -3 to 3
- lateral_bias_five: float32 [256], replicated, may hold values from -3 to 3
- output_three: bfloat16 [3, 3, 256, 256], P(None, None, 'space'), may hold values from -0.125 to 0.125
- output_four: bfloat16 [3, 3, 256, 256], P(None, None, 'space'), may hold values from -0.125 to 0.125
- output_five: bfloat16 [3, 3, 256, 256], P(None, None, 'space'), may hold values from -0.125 to 0.125
- output_bias_three: float32 [256], replicated, may hold values from -3 to 3
- output_bias_four: float32 [256], replicated, may hold values from -3 to 3
- output_bias_five: float32 [256], replicated, may hold values from -3 to 3
Outputs:
- level_three: bfloat16 [16, 128, 128, 256], P('dp', 'space'), parts along dimension 0
- level_four: bfloat16 [16, 64, 64, 256], P('dp', 'space'), parts along dimension 0
- level_five: bfloat16 [16, 32, 32, 256], P('dp'), parts along dimension 0
- level_six: bfloat16 [16, 16, 16, 256], P('dp'), parts along dimension 0
The draws below stay inside these ranges and needn't reach their ends.
There are 16 independent parts, one for each index of `dp`. The reference program is written for one: setup_inputs(seed, part) draws one part's arguments, and reference() takes and returns one part's arrays. A program takes and returns all parts, laid end to end along the dimension named above; an argument that names none is the same for every part. Nothing has to cross between parts.
All inputs are finite; a program needn't handle non-finite values.
Results may differ from the reference program's by a relative error of at most 0.0095.
Values may be sent and summed in bfloat16 or wider, within the bound.
A program may use at most 64 MiB of HBM per device.

```python
import jax
import jax.numpy as jnp

C3 = 512
C4 = 1024
C5 = 2048
FD = 256
IMG = 1
W5 = 32
H5 = 32
H4 = 64
H3 = 128
W4 = 64
W3 = 128


def levels(own_key, shape, shards, low, high):
    gain, own = 1.0, jax.random.fold_in(own_key, 6)
    for dim, shards_of in shards:
        draws = jnp.exp(jax.random.uniform(jax.random.fold_in(own, dim), (shards_of,), jnp.float32, low / len(shards), high / len(shards)))
        gain = gain * jnp.repeat(draws, shape[dim] // shards_of).reshape([-1 if axis == dim else 1 for axis in range(len(shape))])
    return gain


def gaussian(key, shape, width, reach, split=(), dtype=jnp.bfloat16):
    values = width * jax.random.normal(key, shape, jnp.float32)
    if split:
        values = values * levels(key, shape, split, -0.22, 0.18)
    return jnp.clip(values, -reach, reach).astype(dtype)


def setup_inputs(seed: int = 0, part: int = 0) -> dict:
    key_of = jax.random.split(jax.random.key(seed), 16)
    part_keys = jax.random.split(jax.random.fold_in(key_of[15], part), 16)
    section_three = gaussian(part_keys[0], (IMG, H3, W3, C3), 1.0, 6.0, ((1, 16),))
    section_four = gaussian(part_keys[1], (IMG, H4, W4, C4), 1.0, 6.0, ((1, 16),))
    section_five = gaussian(part_keys[2], (IMG, H5, W5, C5), 1.0, 6.0, ((1, 16),))
    lateral_three = gaussian(key_of[3], (C3, FD), C3 ** -0.5, 0.25, ((0, 16),))
    lateral_four = gaussian(key_of[4], (C4, FD), C4 ** -0.5, 0.1875, ((0, 16),))
    lateral_five = gaussian(key_of[5], (C5, FD), C5 ** -0.5, 0.125, ((0, 16),))
    lateral_bias_three = gaussian(key_of[6], (FD,), 0.5, 3.0, (), jnp.float32)
    lateral_bias_four = gaussian(key_of[7], (FD,), 0.5, 3.0, (), jnp.float32)
    lateral_bias_five = gaussian(key_of[8], (FD,), 0.5, 3.0, (), jnp.float32)
    output_three = gaussian(key_of[9], (3, 3, FD, FD), (9 * FD) ** -0.5, 0.125, ((2, 16),))
    output_four = gaussian(key_of[10], (3, 3, FD, FD), (9 * FD) ** -0.5, 0.125, ((2, 16),))
    output_five = gaussian(key_of[11], (3, 3, FD, FD), (9 * FD) ** -0.5, 0.125, ((2, 16),))
    output_bias_three = gaussian(key_of[12], (FD,), 0.5, 3.0, (), jnp.float32)
    output_bias_four = gaussian(key_of[13], (FD,), 0.5, 3.0, (), jnp.float32)
    output_bias_five = gaussian(key_of[14], (FD,), 0.5, 3.0, (), jnp.float32)
    return dict(section_three=section_three, section_four=section_four, section_five=section_five, lateral_three=lateral_three, lateral_four=lateral_four, lateral_five=lateral_five, lateral_bias_three=lateral_bias_three, lateral_bias_four=lateral_bias_four, lateral_bias_five=lateral_bias_five, output_three=output_three, output_four=output_four, output_five=output_five, output_bias_three=output_bias_three, output_bias_four=output_bias_four, output_bias_five=output_bias_five)


def lateral(features, weight, offset):
    images, rows, columns, channels = features.shape
    summed = jnp.dot(features.reshape(-1, channels), weight, preferred_element_type=jnp.float32) + offset
    return summed.reshape(images, rows, columns, -1)


def enlarge(coarse):
    return jnp.repeat(jnp.repeat(coarse, 2, axis=1), 2, axis=2)


def conv_rows(padded, weight, offset):
    images, rows_in, columns, channels = padded.shape
    height = rows_in - 2
    framed = jnp.pad(padded, ((0, 0), (0, 0), (1, 1), (0, 0)))
    summed = jnp.zeros((images * height * columns, weight.shape[3]), jnp.float32)
    for row_off in range(3):
        for col_off in range(3):
            window = framed[:, row_off:row_off + height, col_off:col_off + columns, :].reshape(-1, channels)
            summed = summed + jnp.dot(window, weight[row_off, col_off], preferred_element_type=jnp.float32)
    return (summed + offset).reshape(images, height, columns, -1).astype(jnp.bfloat16)


def pad_rows(field):
    return jnp.pad(field, ((0, 0), (1, 1), (0, 0), (0, 0)))


def reference(section_three, section_four, section_five, lateral_three, lateral_four, lateral_five, lateral_bias_three, lateral_bias_four, lateral_bias_five, output_three, output_four, output_five, output_bias_three, output_bias_four, output_bias_five):
    merged_five = lateral(section_five, lateral_five, lateral_bias_five).astype(jnp.bfloat16)
    merged_four = (lateral(section_four, lateral_four, lateral_bias_four) + enlarge(merged_five).astype(jnp.float32)).astype(jnp.bfloat16)
    merged_three = (lateral(section_three, lateral_three, lateral_bias_three) + enlarge(merged_four).astype(jnp.float32)).astype(jnp.bfloat16)
    level_three = conv_rows(pad_rows(merged_three), output_three, output_bias_three)
    level_four = conv_rows(pad_rows(merged_four), output_four, output_bias_four)
    level_five = conv_rows(pad_rows(merged_five), output_five, output_bias_five)
    level_six = level_five[:, ::2, ::2, :]
    return (level_three, level_four, level_five, level_six)
```

```python
import jax
import jax.numpy as jnp
from jax import lax
from jax.experimental import pallas as pl
from jax.experimental.pallas import tpu as pltpu
from jax.sharding import PartitionSpec as P

MESH = pl.DeviceIdType.MESH
BF16 = jnp.bfloat16
F32 = jnp.float32

L5, L4, L3, W5, W3, W4, ROWS = 0, 128, 192, 224, 368, 512, 656
STAGES = ((L5, L4), (L4, W5), (W5, W3), (W3, W4), (W4, ROWS))
PER_STAGE = 12


def half_rows(first, last):
    return first + (((last - first) // 2 + 15) // 16) * 16


def kernel(
    s3, s4, s5, l3, l4, l5, lb3, lb4, lb5, o3, o4, o5, ob3, ob4, ob5,
    out3, out4, out5, out6,
    x3, x4, x5, held, taps, m3, m4, m5, wide4, wide3, even, y3, y4, y5, y6,
    own_sem, load_sem, send, recv, m_send, m_recv, store_sem,
):
    dp, sp = lax.axis_index("dp"), lax.axis_index("space")
    core, x, z_hi = lax.rem(dp, 2), lax.rem(dp // 2, 4), dp // 8
    y, z = sp // 4, lax.rem(sp, 4)

    def pick(for_zero, for_one):
        return for_zero + core * (for_one - for_zero)

    def along_z(by):
        full = lax.rem(z_hi * 4 + z + by + 8, 8)
        return (full // 4) * 8 + x * 2 + core, y * 4 + lax.rem(full, 4)

    def along_y(by):
        return dp, lax.rem(y + by + 4, 4) * 4 + z

    def first_axis(by):
        for_z, for_y = along_z(by), along_y(by)
        return pick(for_z[0], for_y[0]), pick(for_z[1], for_y[1])

    def second_axis(by):
        for_z, for_y = along_z(by), along_y(by)
        return pick(for_y[0], for_z[0]), pick(for_y[1], for_z[1])

    sibling = (dp + 1 - 2 * core, sp)
    a, b = pick(z, y), pick(y, z)
    sib_b = pick(z, y)
    below, above = (dp, lax.rem(sp + 1, 16)), (dp, lax.rem(sp + 15, 16))
    in_line = [(dp, y * 4 + lax.rem(z + i, 4)) for i in (1, 2, 3)]

    own_slot = 4 * b + a
    lanes = pl.ds(pl.multiple_of(core * 128, 128), 128)
    own_loads = []
    for i, (ref, first) in enumerate(((l5, L5), (l4, L4), (l3, L3), (o5, W5), (o3, W3), (o4, W4))):
        count = ref.shape[0]
        own_loads.append(
            pltpu.make_async_copy(
                ref.at[:, lanes], held.at[core, own_slot, first : first + count, :], own_sem.at[i]
            )
        )
    section_loads = [
        pltpu.make_async_copy(ref.at[0], to, load_sem.at[i])
        for i, (ref, to) in enumerate(((s5, x5), (s4, x4), (s3, x3)))
    ]
    for copy in own_loads + section_loads:
        copy.start()
    own_of_stage = ((0,), (1, 2), (3,), (4,), (5,))

    partners = [along_z(1), along_z(-1), along_y(1), along_y(-1), sibling, below, above] + in_line
    barrier = pltpu.get_barrier_semaphore()
    for where in partners:
        pl.semaphore_signal(barrier, inc=1, device_id=where, device_id_type=MESH)

    m5[0] = jnp.zeros_like(m5[0])
    m5[33] = jnp.zeros_like(m5[33])

    pl.semaphore_wait(barrier, len(partners))

    sent = []

    def go(ref, where, stage, index):
        copy = pltpu.make_async_remote_copy(
            src_ref=ref,
            dst_ref=ref,
            send_sem=send.at[stage * PER_STAGE + index],
            recv_sem=recv.at[stage * PER_STAGE + index],
            device_id=where,
            device_id_type=MESH,
        )
        copy.start()
        sent.append(copy)

    def arrived(ref, stage, index):
        pltpu.make_async_remote_copy(
            src_ref=ref,
            dst_ref=ref,
            send_sem=send.at[stage * PER_STAGE + index],
            recv_sem=recv.at[stage * PER_STAGE + index],
            device_id=sibling,
            device_id_type=MESH,
        ).wait_recv()

    def slot(by, first, last):
        return held.at[core, 4 * b + lax.rem(a + by, 4), first:last, :]

    def block(by, first, last, at=0, count=4):
        return held.at[core, pl.ds(4 * lax.rem(b + by, 4) + at, count), first:last, :]

    def step(stage, k):
        first, last = STAGES[stage]
        mid = half_rows(first, last)
        if k == 0:
            for i in own_of_stage[stage]:
                own_loads[i].wait()
            go(slot(0, first, last), first_axis(1), stage, 0)
            go(slot(0, first, last), first_axis(-1), stage, 1)
        elif k == 1:
            arrived(slot(3, first, last), stage, 0)
            go(slot(3, first, mid), first_axis(1), stage, 2)
            arrived(slot(1, first, last), stage, 1)
            go(slot(1, mid, last), first_axis(-1), stage, 3)
        elif k == 2:
            arrived(slot(2, first, mid), stage, 2)
            arrived(slot(2, mid, last), stage, 3)
            go(block(0, first, last), second_axis(1), stage, 4)
            go(block(0, first, last), second_axis(-1), stage, 5)
            go(block(0, first, last), sibling, stage, 8)
        elif k == 3:
            arrived(block(3, first, last), stage, 4)
            go(block(3, first, last, 0, 2), second_axis(1), stage, 6)
            arrived(block(1, first, last), stage, 5)
            go(block(1, first, last, 2, 2), second_axis(-1), stage, 7)
            go(block(3, first, last), sibling, stage, 9)
            go(block(1, first, last), sibling, stage, 10)
        elif k == 4:
            arrived(block(2, first, last, 0, 2), stage, 6)
            arrived(block(2, first, last, 2, 2), stage, 7)
            go(block(2, first, last), sibling, stage, 11)
        else:
            for by, index in ((0, 8), (3, 9), (1, 10), (2, 11)):
                at = 4 * lax.rem(sib_b + by, 4)
                arrived(held.at[1 - core, pl.ds(at, 4), first:last, :], stage, index)

    def weights(first, count, chunks):
        left = jnp.concatenate([held[0, s, first : first + count, :] for s in chunks], axis=0)
        right = jnp.concatenate(
            [held[1, 4 * (s % 4) + s // 4, first : first + count, :] for s in chunks], axis=0
        )
        return jnp.concatenate([left, right], axis=1)

    def lateral(features, first, count):
        per = 256 // count
        total = None
        for start in range(0, 16, per):
            term = jnp.dot(
                features[:, start * count : (start + per) * count],
                weights(first, count, range(start, start + per)),
                preferred_element_type=F32,
            )
            total = term if total is None else total + term
        return total

    def doubled(field, ref):
        count = field.shape[0]
        for h in range(2):
            for odd in range(2):
                ref[h, pl.ds(odd, count, 2), :] = field[:, 128 * h : 128 * h + 128]

    def doubled_rows(ref, first, count):
        return jnp.concatenate([ref[h, first : first + count, :] for h in range(2)], axis=1)

    m_sent = []

    def m_copy(ref, to, where, index):
        return pltpu.make_async_remote_copy(
            src_ref=ref,
            dst_ref=to,
            send_sem=m_send.at[index],
            recv_sem=m_recv.at[index],
            device_id=where,
            device_id_type=MESH,
        )

    def m_go(ref, to, where, index):
        copy = m_copy(ref, to, where, index)
        copy.start()
        m_sent.append(copy)

    def rows5(first, count):
        return m5.at[pl.ds(1 + first, count)]

    def merge_five():
        section_loads[0].wait()
        merged = lateral(x5[...].reshape(64, 2048), L5, 128) + lb5[...]
        rounded = merged.astype(BF16)
        m5[pl.ds(1 + 2 * sp, 2)] = rounded.reshape(2, 32, 256)
        doubled(rounded.astype(F32), wide4)
        for i in (1, 2, 3):
            m_go(rows5(2 * sp, 2), rows5(2 * sp, 2), in_line[i - 1], i - 1)

    def line_done():
        for i in (1, 2, 3):
            ref = rows5(8 * y + 2 * lax.rem(z + 4 - i, 4), 2)
            m_copy(ref, ref, in_line[0], i - 1).wait_recv()
        ref = rows5(8 * y, 8)
        m_go(ref, ref, along_y(1), 3)
        m_go(ref, ref, along_y(-1), 4)

    def column_done():
        left, right = 8 * lax.rem(y + 3, 4), 8 * lax.rem(y + 1, 4)
        m_copy(rows5(left, 8), rows5(left, 8), along_y(1), 3).wait_recv()
        m_go(rows5(left, 4), rows5(left, 4), along_y(1), 5)
        m_copy(rows5(right, 8), rows5(right, 8), along_y(1), 4).wait_recv()
        m_go(rows5(right + 4, 4), rows5(right + 4, 4), along_y(-1), 6)

    def all_five():
        far = 8 * lax.rem(y + 2, 4)
        m_copy(rows5(far, 4), rows5(far, 4), along_y(1), 5).wait_recv()
        m_copy(rows5(far + 4, 4), rows5(far + 4, 4), along_y(1), 6).wait_recv()

    def merge_four_and_three():
        section_loads[1].wait()
        up = jnp.concatenate([doubled_rows(wide4, 64 * (r // 2), 64) for r in range(4)], axis=0)
        merged = lateral(x4[...].reshape(256, 1024), L4, 64) + lb4[...] + up
        rounded = merged.astype(BF16)
        m4[1:5] = rounded.reshape(4, 64, 256)
        m_go(m4.at[4:5], m4.at[0:1], below, 7)
        m_go(m4.at[1:2], m4.at[5:6], above, 8)
        doubled(rounded.astype(F32), wide3)
        section_loads[2].wait()
        for r in (0, 3, 1, 2):
            up = doubled_rows(wide3, 128 * r, 128)
            merged = lateral(x3[2 * r : 2 * r + 2].reshape(256, 512), L3, 32) + lb3[...]
            merged = merged + jnp.concatenate([up, up], axis=0)
            m3[1 + 2 * r : 3 + 2 * r] = merged.astype(BF16).reshape(2, 128, 256)
        m_go(m3.at[8:9], m3.at[0:1], below, 9)
        m_go(m3.at[1:2], m3.at[9:10], above, 10)

    def rims(ref, index, last):
        m_copy(ref.at[0:1], ref.at[0:1], below, index).wait_recv()
        m_copy(ref.at[last : last + 1], ref.at[last : last + 1], below, index + 1).wait_recv()

        @pl.when(sp == 0)
        def _():
            ref[0] = jnp.zeros_like(ref[0])

        @pl.when(sp == 15)
        def _():
            ref[last] = jnp.zeros_like(ref[last])

    def conv(ref, rows, columns, first, offset, each, keep):
        for c in range(3):
            for r in range(3):
                taps[c, 256 * r : 256 * r + 256, :] = weights(first + 16 * (3 * r + c), 16, range(16))
        count = each * columns
        column = lax.rem(lax.broadcasted_iota(jnp.int32, (count, 256), 0), columns)
        for start in range(0, rows, each):
            window = jnp.concatenate(
                [ref[start + r : start + r + each].reshape(count, 256) for r in range(3)], axis=1
            )
            parts = [jnp.dot(window, taps[c], preferred_element_type=F32) for c in range(3)]
            left = jnp.where(column == 0, 0.0, pltpu.roll(parts[0], 1, 0))
            right = jnp.where(column == columns - 1, 0.0, pltpu.roll(parts[2], count - 1, 0))
            summed = parts[1] + offset[...] + left + right
            keep(start, summed.astype(BF16).reshape(each, columns, 256))

    stores = []

    def store(ref, to):
        copy = pltpu.make_async_copy(ref, to, store_sem.at[len(stores)])
        copy.start()
        stores.append(copy)

    def keep5(start, rounded):
        y5[start : start + 8] = rounded
        store(y5.at[start : start + 8], out5.at[0, start : start + 8])
        for r in range(0, 8, 2):
            for h in range(2):
                even[h, 16 * r : 16 * r + 32, :] = rounded[r, :, 128 * h : 128 * h + 128].astype(F32)
        for h in range(2):
            picked = even[h, pl.ds(0, 64, 2), :].astype(BF16).reshape(4, 16, 128)
            y6[start // 2 : start // 2 + 4, :, 128 * h : 128 * h + 128] = picked

    def keep3(start, rounded):
        y3[start : start + 2] = rounded
        store(y3.at[start : start + 2], out3.at[0, start : start + 2])

    def keep4(start, rounded):
        y4[start : start + 4] = rounded
        store(y4.at[start : start + 4], out4.at[0, start : start + 4])

    for slot_of_time in range(9):
        for stage in range(5):
            k = slot_of_time - stage
            if 0 <= k <= 5:
                step(stage, k)
                if k == 5 and stage == 0:
                    merge_five()
                if k == 5 and stage == 1:
                    merge_four_and_three()
                    line_done()
                if k == 5 and stage == 2:
                    column_done()
                if k == 5 and stage == 3:
                    all_five()
                    conv(m5, 32, 32, W5, ob5, 8, keep5)
                    store(y6, out6.at[0])
    rims(m3, 9, 9)
    conv(m3, 8, 128, W3, ob3, 2, keep3)
    step(4, 5)
    rims(m4, 7, 5)
    conv(m4, 4, 64, W4, ob4, 4, keep4)
    for copy in sent + m_sent:
        copy.wait_send()
    for copy in stores:
        copy.wait()


def on_device(
    section_three,
    section_four,
    section_five,
    lateral_three,
    lateral_four,
    lateral_five,
    lateral_bias_three,
    lateral_bias_four,
    lateral_bias_five,
    output_three,
    output_four,
    output_five,
    output_bias_three,
    output_bias_four,
    output_bias_five,
):
    anywhere = pl.BlockSpec(memory_space=pl.ANY)
    in_vmem = pl.BlockSpec(memory_space=pltpu.VMEM)
    row = [bias.reshape(1, 256) for bias in (
        lateral_bias_three, lateral_bias_four, lateral_bias_five,
        output_bias_three, output_bias_four, output_bias_five)]
    dma = pltpu.SemaphoreType.DMA
    return pl.pallas_call(
        kernel,
        out_shape=(
            jax.ShapeDtypeStruct((1, 8, 128, 256), BF16),
            jax.ShapeDtypeStruct((1, 4, 64, 256), BF16),
            jax.ShapeDtypeStruct((1, 32, 32, 256), BF16),
            jax.ShapeDtypeStruct((1, 16, 16, 256), BF16),
        ),
        in_specs=[anywhere] * 6 + [in_vmem] * 3 + [anywhere] * 3 + [in_vmem] * 3,
        out_specs=(anywhere,) * 4,
        scratch_shapes=[
            pltpu.VMEM((8, 128, 512), BF16),
            pltpu.VMEM((4, 64, 1024), BF16),
            pltpu.VMEM((2, 32, 2048), BF16),
            pltpu.VMEM((2, 16, ROWS, 128), BF16),
            pltpu.VMEM((3, 768, 256), BF16),
            pltpu.VMEM((10, 128, 256), BF16),
            pltpu.VMEM((6, 64, 256), BF16),
            pltpu.VMEM((34, 32, 256), BF16),
            pltpu.VMEM((2, 128, 128), F32),
            pltpu.VMEM((2, 512, 128), F32),
            pltpu.VMEM((2, 128, 128), F32),
            pltpu.VMEM((8, 128, 256), BF16),
            pltpu.VMEM((4, 64, 256), BF16),
            pltpu.VMEM((32, 32, 256), BF16),
            pltpu.VMEM((16, 16, 256), BF16),
            dma((6,)),
            dma((3,)),
            dma((len(STAGES) * PER_STAGE,)),
            dma((len(STAGES) * PER_STAGE,)),
            dma((11,)),
            dma((11,)),
            dma((10,)),
        ],
        compiler_params=pltpu.CompilerParams(
            collective_id=0, has_side_effects=True, vmem_limit_bytes=40 * 1024 * 1024
        ),
    )(
        section_three, section_four, section_five,
        lateral_three, lateral_four, lateral_five, row[0], row[1], row[2],
        output_three.reshape(144, 256), output_four.reshape(144, 256),
        output_five.reshape(144, 256), row[3], row[4], row[5],
    )


def solution(mesh):
    return jax.shard_map(
        on_device,
        mesh=mesh,
        in_specs=(
            P("dp", "space", None, None),
            P("dp", "space", None, None),
            P("dp", "space", None, None),
            P("space", None),
            P("space", None),
            P("space", None),
            P(),
            P(),
            P(),
            P(None, None, "space", None),
            P(None, None, "space", None),
            P(None, None, "space", None),
            P(),
            P(),
            P(),
        ),
        out_specs=(
            P("dp", "space", None, None),
            P("dp", "space", None, None),
            P("dp", None, None, None),
            P("dp", None, None, None),
        ),
        check_vma=False,
    )
```

```python
import functools

import jax
import jax.numpy as jnp
from jax import lax
from jax.experimental import pallas as pl
from jax.experimental.pallas import tpu as pltpu
from jax.sharding import PartitionSpec as P

MESH = pl.DeviceIdType.MESH
BF16 = jnp.bfloat16
F32 = jnp.float32

L5, L4, L3, W5, W4A, W3, W4B, PAD, ROWS = 0, 128, 192, 224, 368, 416, 560, 656, 672
WHOLE = {"A": (0, 128), "C": (128, 96)}
QUARTERED = {"P": (224, 48), "Q": (416, 48), "R": (608, 16)}
VMEM_LIMIT = 56 * 1024 * 1024
COPIES = 2 * 31 + 3 * 29
ORDER = [
    "Q0", "P0", "A0", "R0", "C0", "Q1", "P1", "A1", "A2", "A3", "Q2", "R1", "A4", "A5", "P2", "A6", "C1", "C2",
    "A7", "C3", "Q3", "R2", "A8", "M0", "C4", "P3", "C5", "Q4", "C6", "R3", "C7", "P4", "C8", "M1", "H4", "H3",
    "M2", "R4", "Q5", "M3", "Q6", "P5", "R5", "V2", "R6", "P6", "V4", "M4", "V5", "V3",
]


def kernel(
    s3, s4, s5, l3, l4, l5, lb3, lb4, lb5, o3, o4, o5, ob3, ob4, ob5,
    y3, y4, y5, y6,
    x3, x4, x5, held, taps, m3, m4, m5, wide4, wide3, even,
    offsets, own_sem, load_sem, send, recv, m_send, m_recv,
):
    dp, sp = lax.axis_index("dp"), lax.axis_index("space")
    core, x, z_hi = lax.rem(dp, 2), lax.rem(dp // 2, 4), dp // 8
    y, z = sp // 4, lax.rem(sp, 4)

    def along_y(by):
        return dp, lax.rem(y + by + 4, 4) * 4 + z

    def along_x(by):
        return z_hi * 8 + lax.rem(x + by + 4, 4) * 2 + core, sp

    sibling = (dp + 1 - 2 * core, sp)
    below, above = (dp, lax.rem(sp + 1, 16)), (dp, lax.rem(sp + 15, 16))
    in_line = [(dp, y * 4 + lax.rem(z + i, 4)) for i in (1, 2, 3)]

    lanes = pl.ds(pl.multiple_of(core * 128, 128), 128)
    tensors = (
        (l5, 0, L5, L4),
        (l4, 0, L4, L3),
        (l3, 0, L3, W5),
        (o5, 0, W5, W4A),
        (o4, 0, W4A, W3),
        (o3, 0, W3, W4B),
        (o4, 48, W4B, PAD),
        (o4, 0, PAD, ROWS),
    )

    def load_own(number, first, last):
        for ref, skipped, start, end in tensors:
            low, high = max(first, start), min(last, end)
            if low < high:
                pltpu.make_async_copy(
                    ref.at[low - start + skipped : high - start + skipped, lanes],
                    held.at[core, sp, low:high, :],
                    own_sem.at[number],
                ).start()

    stages = list(WHOLE) + list(QUARTERED)
    for name, (first, count) in WHOLE.items():
        load_own(stages.index(name), first, first + count)
    for name, (first, count) in QUARTERED.items():
        for q in range(4):
            at = first + q * count

            @pl.when(x == q)
            def _():
                load_own(stages.index(name), at, at + count)

    section_loads = [
        pltpu.make_async_copy(ref.at[0], to, load_sem.at[i])
        for i, (ref, to) in enumerate(((s5, x5), (s4, x4), (s3, x3)))
    ]
    bias_loads = [
        pltpu.make_async_copy(ref, offsets.at[i : i + 1], load_sem.at[3 + i])
        for i, ref in enumerate((lb3, lb4, lb5, ob3, ob4, ob5))
    ]
    for copy in section_loads + bias_loads:
        copy.start()
    near = [along_y(by) for by in (1, 2, 3)] + [along_x(1), along_x(-1)]
    partners = near + in_line + [sibling]
    barrier = pltpu.get_barrier_semaphore()
    for where in partners:
        pl.semaphore_signal(barrier, inc=1, device_id=where, device_id_type=MESH)

    m5[0] = jnp.zeros_like(m5[0])
    m5[33] = jnp.zeros_like(m5[33])

    for copy in bias_loads:
        copy.wait()
    pl.semaphore_wait(barrier, len(partners))

    sent = []
    numbers = {}

    def copy_of(ref, where, name):
        number = numbers.setdefault(name, len(numbers))
        return pltpu.make_async_remote_copy(
            src_ref=ref,
            dst_ref=ref,
            send_sem=send.at[number],
            recv_sem=recv.at[number],
            device_id=where,
            device_id_type=MESH,
        )

    def go(ref, where, name):
        copy = copy_of(ref, where, name)
        copy.start()
        sent.append(copy)

    def arrived(ref, name):
        copy_of(ref, sibling, name).wait_recv()

    def step(stage, k):
        quartered = stage in QUARTERED
        first, count = QUARTERED[stage] if quartered else WHOLE[stage]

        def rows(by_x=0):
            if not quartered:
                return pl.ds(first, count)
            return pl.ds(pl.multiple_of(first + count * lax.rem(x + by_x, 4), 16), count)

        def slot(by_z, by_y=0, of_core=core):
            at = 4 * lax.rem(y + by_y + 4, 4) + lax.rem(z + by_z + 4, 4)
            return held.at[of_core, at, rows(), :]

        def block(by, by_x=0):
            return held.at[core, pl.ds(4 * lax.rem(y + by, 4), 4), rows(by_x), :]

        def quarter(of_core, by_x):
            return held.at[of_core, :, rows(by_x), :]

        def along_column(i):
            for by in (1, 3) if quartered else (1, 3, 2):
                go(slot(-i), along_y(by), (stage, "y", i, by))

        def half_block(by, at):
            return held.at[core, pl.ds(4 * lax.rem(y + by, 4) + at, 2), rows(), :]

        def pair_along_x(by):
            go(block(by), along_x(1), (stage, "xl", by))
            go(block(by), along_x(-1), (stage, "xr", by))

        if k == 0:
            own = held.at[core, sp, rows(), :]
            pltpu.make_async_copy(own, own, own_sem.at[stages.index(stage)]).wait()
            for i in (1, 2, 3):
                go(own, in_line[i - 1], (stage, "z", i))
            along_column(0)
            if not quartered:
                go(own, sibling, (stage, "c", 0, 0))
        elif not quartered:
            if k <= 3:
                arrived(slot(-k), (stage, "z", k))
                along_column(k)
                go(slot(-k), sibling, (stage, "c", k, 0))
            elif k <= 7:
                for by in (1, 3, 2):
                    arrived(slot(4 - k, -by), (stage, "y", k - 4, by))
                    go(slot(4 - k, -by), sibling, (stage, "c", k - 4, by))
            else:
                for i in range(4):
                    for by in range(4):
                        arrived(slot(-i, -by, 1 - core), (stage, "c", i, by))
        elif k == 1:
            for i in (1, 2, 3):
                arrived(slot(-i), (stage, "z", i))
                along_column(i)
            pair_along_x(0)
        elif k == 2:
            for by, at in ((1, 0), (3, 2)):
                for i in range(4):
                    arrived(slot(-i, -by), (stage, "y", i, by))
                go(half_block(4 - by, at), along_y(by), (stage, "yo", at))
                pair_along_x(4 - by)
        elif k == 3:
            for at in (0, 2):
                arrived(half_block(2, at), (stage, "yo", at))
            pair_along_x(2)
            go(quarter(core, 0), sibling, (stage, "c", 0))
        elif k == 4:
            for by in (0, 3, 1, 2):
                arrived(block(by, 3), (stage, "xl", by))
                if by in (0, 3):
                    go(block(by, 3), along_x(1), (stage, "xo", by))
                arrived(block(by, 1), (stage, "xr", by))
                if by in (1, 2):
                    go(block(by, 1), along_x(-1), (stage, "xo", by))
            go(quarter(core, 3), sibling, (stage, "c", 1))
            go(quarter(core, 1), sibling, (stage, "c", 2))
        elif k == 5:
            for by in (0, 3, 1, 2):
                arrived(block(by, 2), (stage, "xo", by))
            go(quarter(core, 2), sibling, (stage, "c", 3))
        else:
            for i, by_x in enumerate((0, 3, 1, 2)):
                arrived(quarter(1 - core, by_x), (stage, "c", i))

    def weights(first, count, chunks):
        left = jnp.concatenate([held[0, s, first : first + count, :] for s in chunks], axis=0)
        right = jnp.concatenate(
            [held[1, s, first : first + count, :] for s in chunks], axis=0
        )
        return jnp.concatenate([left, right], axis=1)

    def lateral(features, first, count):
        per = 256 // count
        total = None
        for start in range(0, 16, per):
            term = jnp.dot(
                features[:, start * count : (start + per) * count],
                weights(first, count, range(start, start + per)),
                preferred_element_type=F32,
            )
            total = term if total is None else total + term
        return total

    def doubled(field, ref):
        count = field.shape[0]
        for h in range(2):
            for odd in range(2):
                ref[h, pl.ds(odd, count, 2), :] = field[:, 128 * h : 128 * h + 128]

    def doubled_rows(ref, first, count):
        return jnp.concatenate([ref[h, first : first + count, :] for h in range(2)], axis=1)

    m_sent = []

    def m_copy(ref, to, where, index):
        return pltpu.make_async_remote_copy(
            src_ref=ref,
            dst_ref=to,
            send_sem=m_send.at[index],
            recv_sem=m_recv.at[index],
            device_id=where,
            device_id_type=MESH,
        )

    def m_go(ref, to, where, index):
        copy = m_copy(ref, to, where, index)
        copy.start()
        m_sent.append(copy)

    def rows5(first, count):
        return m5.at[pl.ds(1 + first, count)]

    def merge_five():
        section_loads[0].wait()
        merged = lateral(x5[...].reshape(64, 2048), L5, 128) + offsets[2:3]
        rounded = merged.astype(BF16)
        m5[pl.ds(1 + 2 * sp, 2)] = rounded.reshape(2, 32, 256)
        doubled(rounded.astype(F32), wide4)
        own = rows5(2 * sp, 2)
        for i in (1, 2, 3):
            m_go(own, own, in_line[i - 1], i - 1)
        for by in (1, 3, 2):
            m_go(own, own, along_y(by), 2 + by)

    def pass_five(i):
        ref = rows5(8 * y + 2 * lax.rem(z + 4 - i, 4), 2)
        m_copy(ref, ref, sibling, i - 1).wait_recv()
        for by in (1, 3, 2):
            m_go(ref, ref, along_y(by), 2 + 3 * i + by)

    def all_five():
        for i in range(4):
            for by in (1, 3, 2):
                ref = rows5(8 * lax.rem(y + 4 - by, 4) + 2 * lax.rem(z + 4 - i, 4), 2)
                m_copy(ref, ref, sibling, 2 + 3 * i + by).wait_recv()

    def merge_four():
        section_loads[1].wait()
        up = jnp.concatenate([doubled_rows(wide4, 64 * (r // 2), 64) for r in range(4)], axis=0)
        merged = lateral(x4[...].reshape(256, 1024), L4, 64) + offsets[1:2] + up
        rounded = merged.astype(BF16)
        m4[1:5] = rounded.reshape(4, 64, 256)
        m_go(m4.at[4:5], m4.at[0:1], below, 15)
        m_go(m4.at[1:2], m4.at[5:6], above, 16)
        doubled(rounded.astype(F32), wide3)

    def merge_three():
        section_loads[2].wait()
        for r in (0, 3, 1, 2):
            up = doubled_rows(wide3, 128 * r, 128)
            merged = lateral(x3[2 * r : 2 * r + 2].reshape(256, 512), L3, 32) + offsets[0:1]
            merged = merged + jnp.concatenate([up, up], axis=0)
            m3[1 + 2 * r : 3 + 2 * r] = merged.astype(BF16).reshape(2, 128, 256)
        m_go(m3.at[8:9], m3.at[0:1], below, 17)
        m_go(m3.at[1:2], m3.at[9:10], above, 18)

    def rims(ref, index, last):
        m_copy(ref.at[0:1], ref.at[0:1], below, index).wait_recv()
        m_copy(ref.at[last : last + 1], ref.at[last : last + 1], below, index + 1).wait_recv()

        @pl.when(sp == 0)
        def _():
            ref[0] = jnp.zeros_like(ref[0])

        @pl.when(sp == 15)
        def _():
            ref[last] = jnp.zeros_like(ref[last])

    def prepare(level, tap_rows):
        for c in range(3):
            for r in range(3):
                taps[level, c, 256 * r : 256 * r + 256, :] = weights(tap_rows[3 * r + c], 16, range(16))

    def conv(level, ref, starts, columns, offset, each, keep):
        count = each * columns
        column = lax.rem(lax.broadcasted_iota(jnp.int32, (count, 256), 0), columns)
        for start in starts:
            window = jnp.concatenate(
                [ref[start + r : start + r + each].reshape(count, 256) for r in range(3)], axis=1
            )
            parts = [jnp.dot(window, taps[level, c], preferred_element_type=F32) for c in range(3)]
            left = jnp.where(column == 0, 0.0, pltpu.roll(parts[0], 1, 0))
            right = jnp.where(column == columns - 1, 0.0, pltpu.roll(parts[2], count - 1, 0))
            summed = parts[1] + offsets[offset : offset + 1] + left + right
            keep(start, summed.astype(BF16).reshape(each, columns, 256))

    def keep5(start, rounded):
        y5[start : start + 8] = rounded
        for r in range(0, 8, 2):
            for h in range(2):
                even[h, 16 * r : 16 * r + 32, :] = rounded[r, :, 128 * h : 128 * h + 128].astype(F32)
        for h in range(2):
            picked = even[h, pl.ds(0, 64, 2), :].astype(BF16).reshape(4, 16, 128)
            y6[start // 2 : start // 2 + 4, :, 128 * h : 128 * h + 128] = picked

    def keep3(start, rounded):
        y3[start : start + 2] = rounded

    def keep4(start, rounded):
        y4[start : start + 4] = rounded

    def five():
        prepare(2, range(W5, W4A, 16))
        conv(2, m5, range(0, 32, 8), 32, 5, 8, keep5)

    def inner_three():
        prepare(0, range(W3, W4B, 16))
        conv(0, m3, (2, 4), 128, 3, 2, keep3)

    def outer_three():
        rims(m3, 17, 9)
        conv(0, m3, (0, 6), 128, 3, 2, keep3)

    def four():
        prepare(1, [*range(W4A, W3, 16), *range(W4B, PAD, 16)])
        rims(m4, 15, 5)
        conv(1, m4, (0,), 64, 4, 4, keep4)

    others = {
        "M0": merge_five,
        "M1": functools.partial(pass_five, 1),
        "M2": functools.partial(pass_five, 2),
        "M3": functools.partial(pass_five, 3),
        "M4": all_five,
        "H4": merge_four,
        "H3": merge_three,
        "V5": five,
        "V2": inner_three,
        "V3": outer_three,
        "V4": four,
    }
    for name in ORDER:
        if name in others:
            others[name]()
        else:
            step(name[0], int(name[1]))
    for copy in sent + m_sent:
        copy.wait_send()


def mover(a, b, c, d, to_a, to_b, to_c, to_d, sem):
    copies = [
        pltpu.make_async_copy(ref, to.at[0], sem.at[i])
        for i, (ref, to) in enumerate(((a, to_a), (b, to_b), (c, to_c), (d, to_d)))
    ]
    for copy in copies:
        copy.start()
    for copy in copies:
        copy.wait()


def on_device(
    section_three,
    section_four,
    section_five,
    lateral_three,
    lateral_four,
    lateral_five,
    lateral_bias_three,
    lateral_bias_four,
    lateral_bias_five,
    output_three,
    output_four,
    output_five,
    output_bias_three,
    output_bias_four,
    output_bias_five,
):
    anywhere = pl.BlockSpec(memory_space=pl.ANY)
    row = [bias.reshape(1, 256) for bias in (
        lateral_bias_three, lateral_bias_four, lateral_bias_five,
        output_bias_three, output_bias_four, output_bias_five)]
    dma = pltpu.SemaphoreType.DMA
    held_results = pl.pallas_call(
        kernel,
        out_shape=(
            pltpu.VMEM((8, 128, 256), BF16),
            pltpu.VMEM((4, 64, 256), BF16),
            pltpu.VMEM((32, 32, 256), BF16),
            pltpu.VMEM((16, 16, 256), BF16),
        ),
        in_specs=[anywhere] * 15,
        out_specs=(pl.BlockSpec(memory_space=pltpu.VMEM),) * 4,
        scratch_shapes=[
            pltpu.VMEM((8, 128, 512), BF16),
            pltpu.VMEM((4, 64, 1024), BF16),
            pltpu.VMEM((2, 32, 2048), BF16),
            pltpu.VMEM((2, 16, ROWS, 128), BF16),
            pltpu.VMEM((3, 3, 768, 256), BF16),
            pltpu.VMEM((10, 128, 256), BF16),
            pltpu.VMEM((6, 64, 256), BF16),
            pltpu.VMEM((34, 32, 256), BF16),
            pltpu.VMEM((2, 128, 128), F32),
            pltpu.VMEM((2, 512, 128), F32),
            pltpu.VMEM((2, 128, 128), F32),
            pltpu.VMEM((6, 256), F32),
            dma((5,)),
            dma((9,)),
            dma((COPIES,)),
            dma((COPIES,)),
            dma((19,)),
            dma((19,)),
        ],
        compiler_params=pltpu.CompilerParams(
            collective_id=0, has_side_effects=True, vmem_limit_bytes=VMEM_LIMIT
        ),
    )(
        section_three, section_four, section_five,
        lateral_three, lateral_four, lateral_five, row[0], row[1], row[2],
        output_three.reshape(144, 256), output_four.reshape(144, 256),
        output_five.reshape(144, 256), row[3], row[4], row[5],
    )
    return pl.pallas_call(
        mover,
        out_shape=tuple(jax.ShapeDtypeStruct((1, *one.shape), BF16) for one in held_results),
        in_specs=[anywhere] * 4,
        out_specs=(anywhere,) * 4,
        scratch_shapes=[dma((4,))],
        compiler_params=pltpu.CompilerParams(vmem_limit_bytes=1024 * 1024),
    )(*held_results)


def solution(mesh):
    return jax.shard_map(
        on_device,
        mesh=mesh,
        in_specs=(
            P("dp", "space", None, None),
            P("dp", "space", None, None),
            P("dp", "space", None, None),
            P("space", None),
            P("space", None),
            P("space", None),
            P(),
            P(),
            P(),
            P(None, None, "space", None),
            P(None, None, "space", None),
            P(None, None, "space", None),
            P(),
            P(),
            P(),
        ),
        out_specs=(
            P("dp", "space", None, None),
            P("dp", "space", None, None),
            P("dp", None, None, None),
            P("dp", None, None, None),
        ),
        check_vma=False,
    )
```

```python
import functools

import jax
import jax.numpy as jnp
from jax import lax
from jax.experimental import pallas as pl
from jax.experimental.pallas import tpu as pltpu
from jax.sharding import PartitionSpec as P

MESH = pl.DeviceIdType.MESH
BF16 = jnp.bfloat16
F32 = jnp.float32

L5, L4, L3, W5, W4A, W3, W4B, PAD, ROWS = 0, 128, 192, 224, 368, 416, 560, 656, 672
WHOLE = {"A": (0, 128), "C": (128, 96)}
PARTED = {"P": (224, 48, 4), "Q": (416, 48, 4), "R": (608, 32, 2)}
ONE_HOP = ["P", "R"]
VMEM_LIMIT = 56 * 1024 * 1024
COPIES = 160
SETTLED = 16
ORDER = [
    "Q0", "P0", "A0", "C0", "R0", "Q1", "P1", "A1", "A2", "A3", "P2", "A4", "Q2", "C1", "P3", "A5", "A6", "C2",
    "C3", "A7", "R1", "Q3", "A8", "M0", "P4", "C4", "C5", "C6", "C7", "Q4", "R2", "C8", "H4", "M1", "R3", "M2",
    "H3", "M3", "Q5", "R4", "Q6", "T3", "P5", "V2", "R5", "P6", "T4", "T5", "V4", "S0", "M4", "V5", "V3",
]


def kernel(
    s3, s4, s5, l3, l4, l5, lb3, lb4, lb5, o3, o4, o5, ob3, ob4, ob5,
    y3, y4, y5, y6,
    x3, x4, x5, held, taps, m3, m4, m5, wide4, wide3, even,
    offsets, own_sem, load_sem, send, recv, m_send, m_recv,
):
    dp, sp = lax.axis_index("dp"), lax.axis_index("space")
    core, x, z_hi = lax.rem(dp, 2), lax.rem(dp // 2, 4), dp // 8
    y, z = sp // 4, lax.rem(sp, 4)

    def along_y(by):
        return dp, lax.rem(y + by + 4, 4) * 4 + z

    def along_x(by):
        return z_hi * 8 + lax.rem(x + by + 4, 4) * 2 + core, sp

    sibling = (dp + 1 - 2 * core, sp)
    below, above = (dp, lax.rem(sp + 1, 16)), (dp, lax.rem(sp + 15, 16))
    in_line = [(dp, y * 4 + lax.rem(z + i, 4)) for i in (1, 2, 3)]

    near = [along_y(by) for by in (1, 2, 3)] + [along_x(1), along_x(-1)]
    partners = near + in_line + [sibling]
    barrier = pltpu.get_barrier_semaphore()
    for where in partners:
        pl.semaphore_signal(barrier, inc=1, device_id=where, device_id_type=MESH)

    lanes = pl.ds(pl.multiple_of(core * 128, 128), 128)
    tensors = (
        (l5, 0, L5, L4),
        (l4, 0, L4, L3),
        (l3, 0, L3, W5),
        (o5, 0, W5, W4A),
        (o4, 0, W4A, W3),
        (o3, 0, W3, W4B),
        (o4, 48, W4B, PAD),
        (o4, 0, PAD, ROWS),
    )

    def load_own(number, first, last):
        for ref, skipped, start, end in tensors:
            low, high = max(first, start), min(last, end)
            if low < high:
                pltpu.make_async_copy(
                    ref.at[low - start + skipped : high - start + skipped, lanes],
                    held.at[core, sp, low:high, :],
                    own_sem.at[number],
                ).start()

    stages = list(WHOLE) + list(PARTED)
    for name, (first, count) in WHOLE.items():
        load_own(stages.index(name), first, first + count)
    for name, (first, count, parts) in PARTED.items():
        for q in range(parts):
            at = first + q * count

            @pl.when(lax.rem(x, parts) == q)
            def _():
                load_own(stages.index(name), at, at + count)

    section_loads = [
        pltpu.make_async_copy(ref.at[0], to, load_sem.at[i])
        for i, (ref, to) in enumerate(((s5, x5), (s4, x4), (s3, x3)))
    ]
    bias_loads = [
        pltpu.make_async_copy(ref, offsets.at[i : i + 1], load_sem.at[3 + i])
        for i, ref in enumerate((lb3, lb4, lb5, ob3, ob4, ob5))
    ]
    for copy in section_loads + bias_loads:
        copy.start()
    m5[0] = jnp.zeros_like(m5[0])
    m5[33] = jnp.zeros_like(m5[33])

    pl.semaphore_wait(barrier, len(partners))

    sent = []
    numbers = {}

    def copy_of(ref, where, name):
        number = numbers.setdefault(name, len(numbers))
        return pltpu.make_async_remote_copy(
            src_ref=ref,
            dst_ref=ref,
            send_sem=send.at[number],
            recv_sem=recv.at[number],
            device_id=where,
            device_id_type=MESH,
        )

    def go(ref, where, name):
        copy = copy_of(ref, where, name)
        copy.start()
        sent.append(copy)

    def arrived(ref, name):
        copy_of(ref, sibling, name).wait_recv()

    def step(stage, k):
        first, count, parts = PARTED[stage] if stage in PARTED else (*WHOLE[stage], 1)
        one_hop = parts == 1 or stage in ONE_HOP

        def rows(by_x=0):
            if parts == 1:
                return pl.ds(first, count)
            return pl.ds(pl.multiple_of(first + count * lax.rem(x + by_x, parts), 16), count)

        def slot(by_z, by_y=0, of_core=core):
            at = 4 * lax.rem(y + by_y + 4, 4) + lax.rem(z + by_z + 4, 4)
            return held.at[of_core, at, rows(), :]

        def block(by, by_x=0):
            return held.at[core, pl.ds(4 * lax.rem(y + by, 4), 4), rows(by_x), :]

        def part(of_core, by_x):
            return held.at[of_core, :, rows(by_x), :]

        def along_column(i):
            for by in (1, 3, 2) if one_hop else (1, 3):
                go(slot(-i), along_y(by), (stage, "y", i, by))

        def half_block(by, at):
            return held.at[core, pl.ds(4 * lax.rem(y + by, 4) + at, 2), rows(), :]

        def pair_along_x(by):
            if parts == 4 or by in (0, 3):
                go(block(by), along_x(1), (stage, "xl", by))
            if parts == 4 or by in (1, 2):
                go(block(by), along_x(-1), (stage, "xr", by))

        if k == 0:
            own = held.at[core, sp, rows(), :]
            pltpu.make_async_copy(own, own, own_sem.at[stages.index(stage)]).wait()
            for i in (1, 2, 3):
                go(own, in_line[i - 1], (stage, "z", i))
            along_column(0)
            if parts == 1:
                go(own, sibling, (stage, "c", 0, 0))
        elif parts == 1:
            if k <= 3:
                arrived(slot(-k), (stage, "z", k))
                along_column(k)
                go(slot(-k), sibling, (stage, "c", k, 0))
            elif k <= 7:
                for by in (1, 3, 2):
                    arrived(slot(4 - k, -by), (stage, "y", k - 4, by))
                    go(slot(4 - k, -by), sibling, (stage, "c", k - 4, by))
            else:
                for i in range(4):
                    for by in range(4):
                        arrived(slot(-i, -by, 1 - core), (stage, "c", i, by))
        elif k == 1:
            for i in (1, 2, 3):
                arrived(slot(-i), (stage, "z", i))
                along_column(i)
            pair_along_x(0)
        elif k == 2:
            for by, at in ((1, 0), (3, 2)):
                for i in range(4):
                    arrived(slot(-i, -by), (stage, "y", i, by))
                if not one_hop:
                    go(half_block(4 - by, at), along_y(by), (stage, "yo", at))
                pair_along_x(4 - by)
        elif k == 3:
            if one_hop:
                for i in range(4):
                    arrived(slot(-i, -2), (stage, "y", i, 2))
            else:
                for at in (0, 2):
                    arrived(half_block(2, at), (stage, "yo", at))
            pair_along_x(2)
            go(part(core, 0), sibling, (stage, "c", 0))
        elif k == 4 and parts == 2:
            for by in (0, 3, 1, 2):
                arrived(block(by, 1), (stage, "xl" if by in (0, 3) else "xr", by))
            go(part(core, 1), sibling, (stage, "c", 1))
        elif k == 5 and parts == 2:
            for by_x in range(2):
                arrived(part(1 - core, by_x), (stage, "c", by_x))
        elif k == 4:
            for by in (0, 3, 1, 2):
                arrived(block(by, 3), (stage, "xl", by))
                if by in (0, 3):
                    go(block(by, 3), along_x(1), (stage, "xo", by))
                arrived(block(by, 1), (stage, "xr", by))
                if by in (1, 2):
                    go(block(by, 1), along_x(-1), (stage, "xo", by))
            go(part(core, 3), sibling, (stage, "c", 1))
            go(part(core, 1), sibling, (stage, "c", 2))
        elif k == 5:
            for by in (0, 3, 1, 2):
                arrived(block(by, 2), (stage, "xo", by))
            go(part(core, 2), sibling, (stage, "c", 3))
        else:
            for i, by_x in enumerate((0, 3, 1, 2)):
                arrived(part(1 - core, by_x), (stage, "c", i))

    def weights(first, count, chunks):
        left = jnp.concatenate([held[0, s, first : first + count, :] for s in chunks], axis=0)
        right = jnp.concatenate(
            [held[1, s, first : first + count, :] for s in chunks], axis=0
        )
        return jnp.concatenate([left, right], axis=1)

    def lateral(features, first, count):
        per = 256 // count
        total = None
        for start in range(0, 16, per):
            term = jnp.dot(
                features[:, start * count : (start + per) * count],
                weights(first, count, range(start, start + per)),
                preferred_element_type=F32,
            )
            total = term if total is None else total + term
        return total

    def doubled(field, ref):
        count = field.shape[0]
        for h in range(2):
            for odd in range(2):
                ref[h, pl.ds(odd, count, 2), :] = field[:, 128 * h : 128 * h + 128]

    def doubled_rows(ref, first, count):
        return jnp.concatenate([ref[h, first : first + count, :] for h in range(2)], axis=1)

    m_sent = []

    def m_copy(ref, to, where, index):
        return pltpu.make_async_remote_copy(
            src_ref=ref,
            dst_ref=to,
            send_sem=m_send.at[index],
            recv_sem=m_recv.at[index],
            device_id=where,
            device_id_type=MESH,
        )

    def m_go(ref, to, where, index):
        copy = m_copy(ref, to, where, index)
        copy.start()
        m_sent.append(copy)

    def rows5(first, count):
        return m5.at[pl.ds(1 + first, count)]

    def merge_five():
        section_loads[0].wait()
        for copy in bias_loads:
            copy.wait()
        merged = lateral(x5[...].reshape(64, 2048), L5, 128) + offsets[2:3]
        rounded = merged.astype(BF16)
        m5[pl.ds(1 + 2 * sp, 2)] = rounded.reshape(2, 32, 256)
        doubled(rounded.astype(F32), wide4)
        own = rows5(2 * sp, 2)
        for i in (1, 2, 3):
            m_go(own, own, in_line[i - 1], i - 1)
        for by in (1, 3, 2):
            m_go(own, own, along_y(by), 2 + by)

    def pass_five(i):
        ref = rows5(8 * y + 2 * lax.rem(z + 4 - i, 4), 2)
        m_copy(ref, ref, sibling, i - 1).wait_recv()
        for by in (1, 3, 2):
            m_go(ref, ref, along_y(by), 2 + 3 * i + by)

    def all_five():
        for i in range(4):
            for by in (1, 3, 2):
                ref = rows5(8 * lax.rem(y + 4 - by, 4) + 2 * lax.rem(z + 4 - i, 4), 2)
                m_copy(ref, ref, sibling, 2 + 3 * i + by).wait_recv()

    def merge_four():
        section_loads[1].wait()
        up = jnp.concatenate([doubled_rows(wide4, 64 * (r // 2), 64) for r in range(4)], axis=0)
        merged = lateral(x4[...].reshape(256, 1024), L4, 64) + offsets[1:2] + up
        rounded = merged.astype(BF16)
        m4[1:5] = rounded.reshape(4, 64, 256)
        m_go(m4.at[4:5], m4.at[0:1], below, 15)
        m_go(m4.at[1:2], m4.at[5:6], above, 16)
        doubled(rounded.astype(F32), wide3)

    def merge_three():
        section_loads[2].wait()
        for r in (0, 3, 1, 2):
            up = doubled_rows(wide3, 128 * r, 128)
            merged = lateral(x3[2 * r : 2 * r + 2].reshape(256, 512), L3, 32) + offsets[0:1]
            merged = merged + jnp.concatenate([up, up], axis=0)
            m3[1 + 2 * r : 3 + 2 * r] = merged.astype(BF16).reshape(2, 128, 256)
        m_go(m3.at[8:9], m3.at[0:1], below, 17)
        m_go(m3.at[1:2], m3.at[9:10], above, 18)

    def rims(ref, index, last):
        m_copy(ref.at[0:1], ref.at[0:1], below, index).wait_recv()
        m_copy(ref.at[last : last + 1], ref.at[last : last + 1], below, index + 1).wait_recv()

        @pl.when(sp == 0)
        def _():
            ref[0] = jnp.zeros_like(ref[0])

        @pl.when(sp == 15)
        def _():
            ref[last] = jnp.zeros_like(ref[last])

    def prepare(level, tap_rows):
        for c in range(3):
            for r in range(3):
                taps[level, c, 256 * r : 256 * r + 256, :] = weights(tap_rows[3 * r + c], 16, range(16))

    def conv(level, ref, starts, columns, offset, each, keep):
        count = each * columns
        column = lax.rem(lax.broadcasted_iota(jnp.int32, (count, 256), 0), columns)
        for start in starts:
            window = jnp.concatenate(
                [ref[start + r : start + r + each].reshape(count, 256) for r in range(3)], axis=1
            )
            parts = [jnp.dot(window, taps[level, c], preferred_element_type=F32) for c in range(3)]
            left = jnp.where(column == 0, 0.0, pltpu.roll(parts[0], 1, 0))
            right = jnp.where(column == columns - 1, 0.0, pltpu.roll(parts[2], count - 1, 0))
            summed = parts[1] + offsets[offset : offset + 1] + left + right
            keep(start, summed.astype(BF16).reshape(each, columns, 256))

    def keep5(start, rounded):
        y5[start : start + 8] = rounded
        for r in range(0, 8, 2):
            for h in range(2):
                even[h, 16 * r : 16 * r + 32, :] = rounded[r, :, 128 * h : 128 * h + 128].astype(F32)
        for h in range(2):
            picked = even[h, pl.ds(0, 64, 2), :].astype(BF16).reshape(4, 16, 128)
            y6[start // 2 : start // 2 + 4, :, 128 * h : 128 * h + 128] = picked

    def keep3(start, rounded):
        y3[start : start + 2] = rounded

    def keep4(start, rounded):
        y4[start : start + 4] = rounded

    def five():
        conv(2, m5, range(0, 32, 8), 32, 5, 8, keep5)

    def inner_three():
        conv(0, m3, (2, 4), 128, 3, 2, keep3)

    def outer_three():
        rims(m3, 17, 9)
        conv(0, m3, (0, 6), 128, 3, 2, keep3)

    def four():
        rims(m4, 15, 5)
        conv(1, m4, (0,), 64, 4, 4, keep4)

    def settle():
        for copy in sent[:-SETTLED]:
            copy.wait_send()
        del sent[:-SETTLED]

    others = {
        "T5": functools.partial(prepare, 2, range(W5, W4A, 16)),
        "T3": functools.partial(prepare, 0, range(W3, W4B, 16)),
        "T4": functools.partial(prepare, 1, [*range(W4A, W3, 16), *range(W4B, PAD, 16)]),
        "S0": settle,
        "M0": merge_five,
        "M1": functools.partial(pass_five, 1),
        "M2": functools.partial(pass_five, 2),
        "M3": functools.partial(pass_five, 3),
        "M4": all_five,
        "H4": merge_four,
        "H3": merge_three,
        "V5": five,
        "V2": inner_three,
        "V3": outer_three,
        "V4": four,
    }
    for name in ORDER:
        if name in others:
            others[name]()
        else:
            step(name[0], int(name[1]))
    for copy in sent + m_sent:
        copy.wait_send()


def mover(a, b, c, d, to_a, to_b, to_c, to_d, sem):
    copies = [
        pltpu.make_async_copy(ref, to.at[0], sem.at[i])
        for i, (ref, to) in enumerate(((a, to_a), (b, to_b), (c, to_c), (d, to_d)))
    ]
    for copy in copies:
        copy.start()
    for copy in copies:
        copy.wait()


def on_device(
    section_three,
    section_four,
    section_five,
    lateral_three,
    lateral_four,
    lateral_five,
    lateral_bias_three,
    lateral_bias_four,
    lateral_bias_five,
    output_three,
    output_four,
    output_five,
    output_bias_three,
    output_bias_four,
    output_bias_five,
):
    anywhere = pl.BlockSpec(memory_space=pl.ANY)
    row = [bias.reshape(1, 256) for bias in (
        lateral_bias_three, lateral_bias_four, lateral_bias_five,
        output_bias_three, output_bias_four, output_bias_five)]
    dma = pltpu.SemaphoreType.DMA
    held_results = pl.pallas_call(
        kernel,
        out_shape=(
            pltpu.VMEM((8, 128, 256), BF16),
            pltpu.VMEM((4, 64, 256), BF16),
            pltpu.VMEM((32, 32, 256), BF16),
            pltpu.VMEM((16, 16, 256), BF16),
        ),
        in_specs=[anywhere] * 15,
        out_specs=(pl.BlockSpec(memory_space=pltpu.VMEM),) * 4,
        scratch_shapes=[
            pltpu.VMEM((8, 128, 512), BF16),
            pltpu.VMEM((4, 64, 1024), BF16),
            pltpu.VMEM((2, 32, 2048), BF16),
            pltpu.VMEM((2, 16, ROWS, 128), BF16),
            pltpu.VMEM((3, 3, 768, 256), BF16),
            pltpu.VMEM((10, 128, 256), BF16),
            pltpu.VMEM((6, 64, 256), BF16),
            pltpu.VMEM((34, 32, 256), BF16),
            pltpu.VMEM((2, 128, 128), F32),
            pltpu.VMEM((2, 512, 128), F32),
            pltpu.VMEM((2, 128, 128), F32),
            pltpu.VMEM((6, 256), F32),
            dma((5,)),
            dma((9,)),
            dma((COPIES,)),
            dma((COPIES,)),
            dma((19,)),
            dma((19,)),
        ],
        compiler_params=pltpu.CompilerParams(
            collective_id=0, has_side_effects=True, vmem_limit_bytes=VMEM_LIMIT
        ),
    )(
        section_three, section_four, section_five,
        lateral_three, lateral_four, lateral_five, row[0], row[1], row[2],
        output_three.reshape(144, 256), output_four.reshape(144, 256),
        output_five.reshape(144, 256), row[3], row[4], row[5],
    )
    return pl.pallas_call(
        mover,
        out_shape=tuple(jax.ShapeDtypeStruct((1, *one.shape), BF16) for one in held_results),
        in_specs=[anywhere] * 4,
        out_specs=(anywhere,) * 4,
        scratch_shapes=[dma((4,))],
        compiler_params=pltpu.CompilerParams(vmem_limit_bytes=1024 * 1024),
    )(*held_results)


def solution(mesh):
    return jax.shard_map(
        on_device,
        mesh=mesh,
        in_specs=(
            P("dp", "space", None, None),
            P("dp", "space", None, None),
            P("dp", "space", None, None),
            P("space", None),
            P("space", None),
            P("space", None),
            P(),
            P(),
            P(),
            P(None, None, "space", None),
            P(None, None, "space", None),
            P(None, None, "space", None),
            P(),
            P(),
            P(),
        ),
        out_specs=(
            P("dp", "space", None, None),
            P("dp", "space", None, None),
            P("dp", None, None, None),
            P("dp", None, None, None),
        ),
        check_vma=False,
    )
```

```python
import functools

import jax
import jax.numpy as jnp
from jax import lax
from jax.experimental import pallas as pl
from jax.experimental.pallas import tpu as pltpu
from jax.sharding import PartitionSpec as P

MESH = pl.DeviceIdType.MESH
BF16 = jnp.bfloat16
F32 = jnp.float32

L5, L4, L3, W5, W4A, W3, W4B, PAD, ROWS = 0, 128, 192, 224, 368, 416, 560, 656, 672
WHOLE = {"A": (0, 128), "C": (128, 96)}
PARTED = {"P": (224, 48, 4), "Q": (416, 48, 4), "R": (608, 32, 2)}
ONE_HOP = ["P", "R"]
VMEM_LIMIT = 56 * 1024 * 1024
COPIES = 160
SETTLED = 16
ORDER = [
    "Q0", "P0", "A0", "C0", "R0", "Q1", "P1", "A1", "A2", "A3", "P2", "A4", "Q2", "C1", "P3", "A5", "A6", "C2",
    "C3", "A7", "R1", "Q3", "A8", "M0", "P4", "C4", "C5", "C6", "C7", "Q4", "R2", "M1", "C8", "H4", "R3", "M2",
    "H3", "M3", "Q5", "R4", "Q6", "T3", "P5", "V2", "R5", "P6", "T4", "T5", "V4", "S0", "M4", "V5", "V3",
]


def kernel(
    s3, s4, s5, l3, l4, l5, lb3, lb4, lb5, o3, o4, o5, ob3, ob4, ob5,
    y3, y4, y5, y6,
    x3, x4, x5, held, taps, m3, m4, m5, wide4, wide3, even,
    offsets, own_sem, load_sem, send, recv, m_send, m_recv,
):
    dp, sp = lax.axis_index("dp"), lax.axis_index("space")
    core, x, z_hi = lax.rem(dp, 2), lax.rem(dp // 2, 4), dp // 8
    y, z = sp // 4, lax.rem(sp, 4)

    def along_y(by):
        return dp, lax.rem(y + by + 4, 4) * 4 + z

    def along_x(by):
        return z_hi * 8 + lax.rem(x + by + 4, 4) * 2 + core, sp

    sibling = (dp + 1 - 2 * core, sp)
    below, above = (dp, lax.rem(sp + 1, 16)), (dp, lax.rem(sp + 15, 16))
    in_line = [(dp, y * 4 + lax.rem(z + i, 4)) for i in (1, 2, 3)]

    near = [along_y(by) for by in (1, 2, 3)] + [along_x(1), along_x(-1)]
    partners = near + in_line + [sibling]
    barrier = pltpu.get_barrier_semaphore()
    for where in partners:
        pl.semaphore_signal(barrier, inc=1, device_id=where, device_id_type=MESH)

    lanes = pl.ds(pl.multiple_of(core * 128, 128), 128)
    tensors = (
        (l5, 0, L5, L4),
        (l4, 0, L4, L3),
        (l3, 0, L3, W5),
        (o5, 0, W5, W4A),
        (o4, 0, W4A, W3),
        (o3, 0, W3, W4B),
        (o4, 48, W4B, PAD),
        (o4, 0, PAD, ROWS),
    )

    def load_own(number, first, last):
        for ref, skipped, start, end in tensors:
            low, high = max(first, start), min(last, end)
            if low < high:
                pltpu.make_async_copy(
                    ref.at[low - start + skipped : high - start + skipped, lanes],
                    held.at[core, sp, low:high, :],
                    own_sem.at[number],
                ).start()

    stages = list(WHOLE) + list(PARTED)
    for name, (first, count) in WHOLE.items():
        load_own(stages.index(name), first, first + count)
    for name, (first, count, parts) in PARTED.items():
        for q in range(parts):
            at = first + q * count

            @pl.when(lax.rem(x, parts) == q)
            def _():
                load_own(stages.index(name), at, at + count)

    section_loads = [
        pltpu.make_async_copy(ref.at[0], to, load_sem.at[i])
        for i, (ref, to) in enumerate(((s5, x5), (s4, x4), (s3, x3)))
    ]
    bias_loads = [
        pltpu.make_async_copy(ref, offsets.at[i : i + 1], load_sem.at[3 + i])
        for i, ref in enumerate((lb3, lb4, lb5, ob3, ob4, ob5))
    ]
    for copy in section_loads + bias_loads:
        copy.start()
    m5[0] = jnp.zeros_like(m5[0])
    m5[33] = jnp.zeros_like(m5[33])

    pl.semaphore_wait(barrier, len(partners))

    sent = []
    numbers = {}

    def copy_of(ref, where, name):
        number = numbers.setdefault(name, len(numbers))
        return pltpu.make_async_remote_copy(
            src_ref=ref,
            dst_ref=ref,
            send_sem=send.at[number],
            recv_sem=recv.at[number],
            device_id=where,
            device_id_type=MESH,
        )

    def go(ref, where, name):
        copy = copy_of(ref, where, name)
        copy.start()
        sent.append(copy)

    def arrived(ref, name):
        copy_of(ref, sibling, name).wait_recv()

    def step(stage, k):
        first, count, parts = PARTED[stage] if stage in PARTED else (*WHOLE[stage], 1)
        one_hop = parts == 1 or stage in ONE_HOP

        def rows(by_x=0):
            if parts == 1:
                return pl.ds(first, count)
            return pl.ds(pl.multiple_of(first + count * lax.rem(x + by_x, parts), 16), count)

        def slot(by_z, by_y=0, of_core=core):
            at = 4 * lax.rem(y + by_y + 4, 4) + lax.rem(z + by_z + 4, 4)
            return held.at[of_core, at, rows(), :]

        def block(by, by_x=0):
            return held.at[core, pl.ds(4 * lax.rem(y + by, 4), 4), rows(by_x), :]

        def part(of_core, by_x):
            return held.at[of_core, :, rows(by_x), :]

        def along_column(i):
            for by in (1, 3, 2) if one_hop else (1, 3):
                go(slot(-i), along_y(by), (stage, "y", i, by))

        def half_block(by, at):
            return held.at[core, pl.ds(4 * lax.rem(y + by, 4) + at, 2), rows(), :]

        def pair_along_x(by):
            if parts == 4 or by in (0, 3):
                go(block(by), along_x(1), (stage, "xl", by))
            if parts == 4 or by in (1, 2):
                go(block(by), along_x(-1), (stage, "xr", by))

        if k == 0:
            own = held.at[core, sp, rows(), :]
            pltpu.make_async_copy(own, own, own_sem.at[stages.index(stage)]).wait()
            for i in (1, 2, 3):
                go(own, in_line[i - 1], (stage, "z", i))
            along_column(0)
            if parts == 1:
                go(own, sibling, (stage, "c", 0, 0))
        elif parts == 1:
            if k <= 3:
                arrived(slot(-k), (stage, "z", k))
                along_column(k)
                go(slot(-k), sibling, (stage, "c", k, 0))
            elif k <= 7:
                for by in (1, 3, 2):
                    arrived(slot(4 - k, -by), (stage, "y", k - 4, by))
                    go(slot(4 - k, -by), sibling, (stage, "c", k - 4, by))
            else:
                for i in range(4):
                    for by in range(4):
                        arrived(slot(-i, -by, 1 - core), (stage, "c", i, by))
        elif k == 1:
            for i in (1, 2, 3):
                arrived(slot(-i), (stage, "z", i))
                along_column(i)
            pair_along_x(0)
        elif k == 2:
            for by, at in ((1, 0), (3, 2)):
                for i in range(4):
                    arrived(slot(-i, -by), (stage, "y", i, by))
                if not one_hop:
                    go(half_block(4 - by, at), along_y(by), (stage, "yo", at))
                pair_along_x(4 - by)
        elif k == 3:
            if one_hop:
                for i in range(4):
                    arrived(slot(-i, -2), (stage, "y", i, 2))
            else:
                for at in (0, 2):
                    arrived(half_block(2, at), (stage, "yo", at))
            pair_along_x(2)
            go(part(core, 0), sibling, (stage, "c", 0))
        elif k == 4 and parts == 2:
            for by in (0, 3, 1, 2):
                arrived(block(by, 1), (stage, "xl" if by in (0, 3) else "xr", by))
            go(part(core, 1), sibling, (stage, "c", 1))
        elif k == 5 and parts == 2:
            for by_x in range(2):
                arrived(part(1 - core, by_x), (stage, "c", by_x))
        elif k == 4:
            for by in (0, 3, 1, 2):
                arrived(block(by, 3), (stage, "xl", by))
                if by in (0, 3):
                    go(block(by, 3), along_x(1), (stage, "xo", by))
                arrived(block(by, 1), (stage, "xr", by))
                if by in (1, 2):
                    go(block(by, 1), along_x(-1), (stage, "xo", by))
            go(part(core, 3), sibling, (stage, "c", 1))
            go(part(core, 1), sibling, (stage, "c", 2))
        elif k == 5:
            for by in (0, 3, 1, 2):
                arrived(block(by, 2), (stage, "xo", by))
            go(part(core, 2), sibling, (stage, "c", 3))
        else:
            for i, by_x in enumerate((0, 3, 1, 2)):
                arrived(part(1 - core, by_x), (stage, "c", i))

    def weights(first, count, chunks):
        left = jnp.concatenate([held[0, s, first : first + count, :] for s in chunks], axis=0)
        right = jnp.concatenate(
            [held[1, s, first : first + count, :] for s in chunks], axis=0
        )
        return jnp.concatenate([left, right], axis=1)

    def lateral(features, first, count):
        per = 256 // count
        total = None
        for start in range(0, 16, per):
            term = jnp.dot(
                features[:, start * count : (start + per) * count],
                weights(first, count, range(start, start + per)),
                preferred_element_type=F32,
            )
            total = term if total is None else total + term
        return total

    def doubled(field, ref):
        count = field.shape[0]
        for h in range(2):
            for odd in range(2):
                ref[h, pl.ds(odd, count, 2), :] = field[:, 128 * h : 128 * h + 128]

    def doubled_rows(ref, first, count):
        return jnp.concatenate([ref[h, first : first + count, :] for h in range(2)], axis=1)

    m_sent = []

    def m_copy(ref, to, where, index):
        return pltpu.make_async_remote_copy(
            src_ref=ref,
            dst_ref=to,
            send_sem=m_send.at[index],
            recv_sem=m_recv.at[index],
            device_id=where,
            device_id_type=MESH,
        )

    def m_go(ref, to, where, index):
        copy = m_copy(ref, to, where, index)
        copy.start()
        m_sent.append(copy)

    def rows5(first, count):
        return m5.at[pl.ds(1 + first, count)]

    def merge_five():
        section_loads[0].wait()
        for copy in bias_loads:
            copy.wait()
        merged = lateral(x5[...].reshape(64, 2048), L5, 128) + offsets[2:3]
        rounded = merged.astype(BF16)
        m5[pl.ds(1 + 2 * sp, 2)] = rounded.reshape(2, 32, 256)
        doubled(rounded.astype(F32), wide4)
        own = rows5(2 * sp, 2)
        for i in (1, 2, 3):
            m_go(own, own, in_line[i - 1], i - 1)
        for by in (1, 3, 2):
            m_go(own, own, along_y(by), 2 + by)

    def pass_five(i):
        ref = rows5(8 * y + 2 * lax.rem(z + 4 - i, 4), 2)
        m_copy(ref, ref, sibling, i - 1).wait_recv()
        for by in (1, 3, 2):
            m_go(ref, ref, along_y(by), 2 + 3 * i + by)

    def all_five():
        for i in range(4):
            for by in (1, 3, 2):
                ref = rows5(8 * lax.rem(y + 4 - by, 4) + 2 * lax.rem(z + 4 - i, 4), 2)
                m_copy(ref, ref, sibling, 2 + 3 * i + by).wait_recv()

    def merge_four():
        section_loads[1].wait()
        up = jnp.concatenate([doubled_rows(wide4, 64 * (r // 2), 64) for r in range(4)], axis=0)
        merged = lateral(x4[...].reshape(256, 1024), L4, 64) + offsets[1:2] + up
        rounded = merged.astype(BF16)
        m4[1:5] = rounded.reshape(4, 64, 256)
        m_go(m4.at[4:5], m4.at[0:1], below, 15)
        m_go(m4.at[1:2], m4.at[5:6], above, 16)
        doubled(rounded.astype(F32), wide3)

    def merge_three():
        section_loads[2].wait()
        for r in (0, 3, 1, 2):
            up = doubled_rows(wide3, 128 * r, 128)
            merged = lateral(x3[2 * r : 2 * r + 2].reshape(256, 512), L3, 32) + offsets[0:1]
            merged = merged + jnp.concatenate([up, up], axis=0)
            m3[1 + 2 * r : 3 + 2 * r] = merged.astype(BF16).reshape(2, 128, 256)
        m_go(m3.at[8:9], m3.at[0:1], below, 17)
        m_go(m3.at[1:2], m3.at[9:10], above, 18)

    def rims(ref, index, last):
        m_copy(ref.at[0:1], ref.at[0:1], below, index).wait_recv()
        m_copy(ref.at[last : last + 1], ref.at[last : last + 1], below, index + 1).wait_recv()

        @pl.when(sp == 0)
        def _():
            ref[0] = jnp.zeros_like(ref[0])

        @pl.when(sp == 15)
        def _():
            ref[last] = jnp.zeros_like(ref[last])

    def prepare(level, tap_rows):
        for c in range(3):
            for r in range(3):
                taps[level, c, 256 * r : 256 * r + 256, :] = weights(tap_rows[3 * r + c], 16, range(16))

    def conv(level, ref, starts, columns, offset, each, keep):
        count = each * columns
        column = lax.rem(lax.broadcasted_iota(jnp.int32, (count, 256), 0), columns)
        for start in starts:
            window = jnp.concatenate(
                [ref[start + r : start + r + each].reshape(count, 256) for r in range(3)], axis=1
            )
            parts = [jnp.dot(window, taps[level, c], preferred_element_type=F32) for c in range(3)]
            left = jnp.where(column == 0, 0.0, pltpu.roll(parts[0], 1, 0))
            right = jnp.where(column == columns - 1, 0.0, pltpu.roll(parts[2], count - 1, 0))
            summed = parts[1] + offsets[offset : offset + 1] + left + right
            keep(start, summed.astype(BF16).reshape(each, columns, 256))

    def keep5(start, rounded):
        y5[start : start + 8] = rounded
        for r in range(0, 8, 2):
            for h in range(2):
                even[h, 16 * r : 16 * r + 32, :] = rounded[r, :, 128 * h : 128 * h + 128].astype(F32)
        for h in range(2):
            picked = even[h, pl.ds(0, 64, 2), :].astype(BF16).reshape(4, 16, 128)
            y6[start // 2 : start // 2 + 4, :, 128 * h : 128 * h + 128] = picked

    def keep3(start, rounded):
        y3[start : start + 2] = rounded

    def keep4(start, rounded):
        y4[start : start + 4] = rounded

    def five():
        conv(2, m5, range(0, 32, 8), 32, 5, 8, keep5)

    def inner_three():
        conv(0, m3, (2, 4), 128, 3, 2, keep3)

    def outer_three():
        rims(m3, 17, 9)
        conv(0, m3, (0, 6), 128, 3, 2, keep3)

    def four():
        rims(m4, 15, 5)
        conv(1, m4, (0,), 64, 4, 4, keep4)

    def settle():
        for copy in sent[:-SETTLED]:
            copy.wait_send()
        del sent[:-SETTLED]

    others = {
        "T5": functools.partial(prepare, 2, range(W5, W4A, 16)),
        "T3": functools.partial(prepare, 0, range(W3, W4B, 16)),
        "T4": functools.partial(prepare, 1, [*range(W4A, W3, 16), *range(W4B, PAD, 16)]),
        "S0": settle,
        "M0": merge_five,
        "M1": functools.partial(pass_five, 1),
        "M2": functools.partial(pass_five, 2),
        "M3": functools.partial(pass_five, 3),
        "M4": all_five,
        "H4": merge_four,
        "H3": merge_three,
        "V5": five,
        "V2": inner_three,
        "V3": outer_three,
        "V4": four,
    }
    for name in ORDER:
        if name in others:
            others[name]()
        else:
            step(name[0], int(name[1]))
    for copy in sent + m_sent:
        copy.wait_send()


def mover(a, b, c, d, to_a, to_b, to_c, to_d, sem):
    copies = [
        pltpu.make_async_copy(ref, to.at[0], sem.at[i])
        for i, (ref, to) in enumerate(((a, to_a), (b, to_b), (c, to_c), (d, to_d)))
    ]
    for copy in copies:
        copy.start()
    for copy in copies:
        copy.wait()


def on_device(
    section_three,
    section_four,
    section_five,
    lateral_three,
    lateral_four,
    lateral_five,
    lateral_bias_three,
    lateral_bias_four,
    lateral_bias_five,
    output_three,
    output_four,
    output_five,
    output_bias_three,
    output_bias_four,
    output_bias_five,
):
    anywhere = pl.BlockSpec(memory_space=pl.ANY)
    row = [bias.reshape(1, 256) for bias in (
        lateral_bias_three, lateral_bias_four, lateral_bias_five,
        output_bias_three, output_bias_four, output_bias_five)]
    dma = pltpu.SemaphoreType.DMA
    held_results = pl.pallas_call(
        kernel,
        out_shape=(
            pltpu.VMEM((8, 128, 256), BF16),
            pltpu.VMEM((4, 64, 256), BF16),
            pltpu.VMEM((32, 32, 256), BF16),
            pltpu.VMEM((16, 16, 256), BF16),
        ),
        in_specs=[anywhere] * 15,
        out_specs=(pl.BlockSpec(memory_space=pltpu.VMEM),) * 4,
        scratch_shapes=[
            pltpu.VMEM((8, 128, 512), BF16),
            pltpu.VMEM((4, 64, 1024), BF16),
            pltpu.VMEM((2, 32, 2048), BF16),
            pltpu.VMEM((2, 16, ROWS, 128), BF16),
            pltpu.VMEM((3, 3, 768, 256), BF16),
            pltpu.VMEM((10, 128, 256), BF16),
            pltpu.VMEM((6, 64, 256), BF16),
            pltpu.VMEM((34, 32, 256), BF16),
            pltpu.VMEM((2, 128, 128), F32),
            pltpu.VMEM((2, 512, 128), F32),
            pltpu.VMEM((2, 128, 128), F32),
            pltpu.VMEM((6, 256), F32),
            dma((5,)),
            dma((9,)),
            dma((COPIES,)),
            dma((COPIES,)),
            dma((19,)),
            dma((19,)),
        ],
        compiler_params=pltpu.CompilerParams(
            collective_id=0, has_side_effects=True, vmem_limit_bytes=VMEM_LIMIT
        ),
    )(
        section_three, section_four, section_five,
        lateral_three, lateral_four, lateral_five, row[0], row[1], row[2],
        output_three.reshape(144, 256), output_four.reshape(144, 256),
        output_five.reshape(144, 256), row[3], row[4], row[5],
    )
    return pl.pallas_call(
        mover,
        out_shape=tuple(jax.ShapeDtypeStruct((1, *one.shape), BF16) for one in held_results),
        in_specs=[anywhere] * 4,
        out_specs=(anywhere,) * 4,
        scratch_shapes=[dma((4,))],
        compiler_params=pltpu.CompilerParams(vmem_limit_bytes=1024 * 1024),
    )(*held_results)


def solution(mesh):
    return jax.shard_map(
        on_device,
        mesh=mesh,
        in_specs=(
            P("dp", "space", None, None),
            P("dp", "space", None, None),
            P("dp", "space", None, None),
            P("space", None),
            P("space", None),
            P("space", None),
            P(),
            P(),
            P(),
            P(None, None, "space", None),
            P(None, None, "space", None),
            P(None, None, "space", None),
            P(),
            P(),
            P(),
        ),
        out_specs=(
            P("dp", "space", None, None),
            P("dp", "space", None, None),
            P("dp", None, None, None),
            P("dp", None, None, None),
        ),
        check_vma=False,
    )
```
